32 devices in a mesh: row: 4 (over y, core), col: 8 (over z, x).
Axes of the slice: x: 2, y: 2, z: 4, core: 2. Of those that a mesh axis runs over, the one named last changes fastest.
Arguments:
- tokens: bfloat16 [512, 8192], P('col', 'row'), may hold values from -6 to 6
- norm_gain: float32 [8192], P('row'), may hold values from 0.1 to 1.9
- gate_weight: bfloat16 [8192, 28672], P('row', 'col'), may hold values from -0.0625 to 0.0625
- up_weight: bfloat16 [8192, 28672], P('row', 'col'), may hold values from -0.0625 to 0.0625
- down_weight: bfloat16 [28672, 8192], P('col', 'row'), may hold values from -0.03125 to 0.03125
Outputs:
- block_out: bfloat16 [512, 8192], P('col', 'row')
The draws below stay inside these ranges and needn't reach their ends.
All inputs are finite; a program needn't handle non-finite values.
Results may differ from the reference program's by a relative error of at most 0.0017.
Values may be sent and summed in bfloat16 or wider, within the bound.
A program may use at most 128 MiB of HBM per device.

```python
import jax
import jax.numpy as jnp
from jax import lax

D = 8192
FF = 28672
TOKENS = 512


def level_of(own_key, dims, split, low, high):
    factor_of, own = 1.0, jax.random.fold_in(own_key, 6)
    for dim, blocks in split:
        steps = jnp.exp(jax.random.uniform(jax.random.fold_in(own, dim), (blocks,), jnp.float32, low / len(split), high / len(split)))
        factor_of = factor_of * jnp.repeat(steps, dims[dim] // blocks).reshape([-1 if axis == dim else 1 for axis in range(len(dims))])
    return factor_of


def normal_values(own_key, dims, spread, reach, pieces=(), held_as=jnp.bfloat16):
    loudness = level_of(own_key, dims, pieces, -0.22, 0.18) if pieces else 1.0
    drawn = jax.random.normal(own_key, dims, jnp.float32) * spread * loudness
    return jnp.minimum(jnp.maximum(drawn, -reach), reach).astype(held_as)


def setup_inputs(seed: int = 0) -> dict:
    splits = jax.random.split(jax.random.key(seed), 6)
    return {
        "tokens": normal_values(splits[0], (TOKENS, D), 1.0, 6.0, ((0, 8), (1, 4))),
        "norm_gain": jnp.clip(1.0 + 0.18 * jax.random.normal(splits[1], (D,), jnp.float32), 0.1, 1.9),
        "gate_weight": normal_values(splits[2], (D, FF), D ** -0.5, 0.0625, ((0, 4), (1, 8))),
        "up_weight": normal_values(splits[3], (D, FF), D ** -0.5, 0.0625, ((0, 4), (1, 8))),
        "down_weight": normal_values(splits[4], (FF, D), FF ** -0.5, 0.03125, ((0, 8), (1, 4))),
    }


def reference(tokens, norm_gain, gate_weight, up_weight, down_weight):
    values = tokens.astype(jnp.float32)
    mean_sq = lax.optimization_barrier(jnp.sum(values * values, axis=1, keepdims=True)) / D
    normed = (values * lax.rsqrt(mean_sq + 1e-05) * norm_gain.astype(jnp.float32)[None, :]).astype(jnp.bfloat16)
    gate_sum = jnp.dot(normed, gate_weight, preferred_element_type=jnp.float32)
    up_sum = jnp.dot(normed, up_weight, preferred_element_type=jnp.float32)
    hidden = (jax.nn.silu(gate_sum) * up_sum).astype(jnp.bfloat16)
    branch = jnp.dot(hidden, down_weight, preferred_element_type=jnp.float32)
    return (values + branch).astype(jnp.bfloat16)
```

```python
import functools

import jax
import jax.numpy as jnp
from jax import lax
from jax.experimental import pallas as pl
from jax.experimental.pallas import tpu as pltpu
from jax.sharding import PartitionSpec as P

MESH = pl.DeviceIdType.MESH
D = 8192
TILES = 7
CORES = 2
PASSES = 2
VMEM_LIMIT = 67043328


epsilon = 1e-05


def block_kernel(
    rows, xs, zs,
    tokens, gain, gate_hbm, up_hbm, down_hbm, out,
    squares_out, squares_in, normed, gate_buf, up_buf, down_buf, part, from_core, sums_out, sums_in, hid,
    acc, x_in, z_out, z_in,
    s_send, s_recv, ga_send, ga_recv, gb_send, gb_recv, w_sem, d_sem, core_send, core_recv, y_send, y_recv,
    h_send, h_recv, p_send, p_recv, rx_send, rx_recv, rz_send, rz_recv,
):
    chips = rows // CORES
    me = lax.axis_index("row")
    y, core = me // CORES, me % CORES
    partner = y * CORES + (1 - core)
    at = lax.axis_index("col")
    z, x = at // xs, at % xs
    count = tokens.shape[0]
    piece = count // PASSES
    line = zs * piece
    span = normed.shape[1]
    half, block = span // CORES, span // rows
    width = gate_buf.shape[2]
    total_steps = PASSES * TILES

    def remote(src, dst, send, recv, device):
        return pltpu.make_async_remote_copy(src, dst, send, recv, device_id=device, device_id_type=MESH)

    def peer(d):
        return lax.rem(y + d, chips)

    def z_peer(d):
        return {"col": lax.rem(z + d, zs) * xs + x}

    def x_peer(e):
        return {"col": z * xs + lax.rem(x + e, xs)}

    def spot(to_x, to_z):
        return pl.ds(pl.multiple_of(to_x * line + to_z * piece, piece), piece)

    def line_of(to_x):
        return pl.ds(pl.multiple_of(to_x * line, line), line)

    def mine(chip):
        return pl.ds(pl.multiple_of(core * half + chip * block, block), block)

    def weights(u):
        slot = lax.rem(u, 2)
        columns = pl.ds(pl.multiple_of(lax.rem(u, TILES) * width, width), width)
        return (
            pltpu.make_async_copy(gate_hbm.at[:, columns], gate_buf.at[slot], w_sem.at[slot, 0]),
            pltpu.make_async_copy(up_hbm.at[:, columns], up_buf.at[slot], w_sem.at[slot, 1]),
        )

    def down_weights(u):
        slot = lax.rem(u, 2)
        lines = pl.ds(pl.multiple_of(lax.rem(u, TILES) * width, width), width)
        return pltpu.make_async_copy(down_hbm.at[lines, :], down_buf.at[slot], d_sem.at[slot])

    def s_copy(d):
        return remote(squares_out, squares_in.at[d - 1], s_send.at[d - 1], s_recv.at[d - 1],
                      {"row": lax.rem(me + d, rows)})

    def ga_copy(p, d):
        return remote(normed.at[p, spot(x, z)], normed.at[p, spot(x, z)],
                      ga_send.at[p, d - 1], ga_recv.at[p, d - 1], z_peer(d))

    def gb_copy(p, e):
        return remote(normed.at[p, line_of(x)], normed.at[p, line_of(x)],
                      gb_send.at[p, e - 1], gb_recv.at[p, e - 1], x_peer(e))

    def rx_copy(p, e):
        return remote(acc.at[p, line_of(lax.rem(x + e, xs))], x_in.at[p, e - 1],
                      rx_send.at[p, e - 1], rx_recv.at[p, e - 1], x_peer(e))

    def rz_copy(p, d):
        return remote(z_out.at[p, d - 1], z_in.at[p, d - 1],
                      rz_send.at[p, d - 1], rz_recv.at[p, d - 1], z_peer(d))

    def core_copy(u):
        other = pl.ds(pl.multiple_of((1 - core) * half, half), half)
        return remote(part.at[u, other], from_core.at[u], core_send.at[u], core_recv.at[u], {"row": partner})

    def y_copy(u, d):
        return remote(sums_out.at[u, d - 1], sums_in.at[u, d - 1], y_send.at[u, d - 1], y_recv.at[u, d - 1],
                      {"row": peer(d) * CORES + core})

    def h_copy(u, d):
        return remote(hid.at[u, mine(y)], hid.at[u, mine(y)], h_send.at[u, d - 1], h_recv.at[u, d - 1],
                      {"row": peer(d) * CORES + core})

    def p_copy(u, d):
        source = lax.rem(y + chips - d, chips)
        return remote(hid.at[u, mine(source)], hid.at[u, mine(source)], p_send.at[u, d], p_recv.at[u, d],
                      {"row": partner})

    for copy in weights(0):
        copy.start()
    down_weights(0).start()

    values = tokens[...].astype(jnp.float32)
    own_squares = jnp.sum(values * values, axis=1, keepdims=True)
    squares_out[...] = jnp.broadcast_to(own_squares, squares_out.shape)

    barrier = pltpu.get_barrier_semaphore()
    for d in range(1, rows):
        pl.semaphore_signal(barrier, inc=1, device_id={"row": lax.rem(me + d, rows)}, device_id_type=MESH)
    for d in range(1, zs):
        pl.semaphore_signal(barrier, inc=1, device_id=z_peer(d), device_id_type=MESH)
    for e in range(1, xs):
        pl.semaphore_signal(barrier, inc=1, device_id=x_peer(e), device_id_type=MESH)
    pl.semaphore_wait(barrier, rows + zs + xs - 3)

    for d in range(1, rows):
        s_copy(d).start()
    squares = squares_out[...]
    for d in range(1, rows):
        s_copy(d).wait_recv()
        squares += squares_in[d - 1]
    factor = lax.rsqrt(squares[:, :1] / D + epsilon)
    scaled = (values * factor * gain[...]).astype(jnp.bfloat16)

    def gather_z(p):
        for d in range(1, zs):
            ga_copy(p, d).start()

    def gather_x(p):
        for d in range(1, zs):
            ga_copy(p, d).wait_recv()
        for e in range(1, xs):
            gb_copy(p, e).start()

    def gather_end(p):
        for e in range(1, xs):
            gb_copy(p, e).wait_recv()

    def scatter_x(p):
        for e in range(1, xs):
            rx_copy(p, e).start()

    def line_sum(p, to_z):
        value = acc[p, spot(x, to_z), :]
        near = pl.ds(pl.multiple_of(to_z * piece, piece), piece)
        for e in range(1, xs):
            value += x_in[p, e - 1, near, :]
        return value

    def scatter_z(p):
        for e in range(1, xs):
            rx_copy(p, e).wait_recv()
        for d in range(1, zs):
            z_out[p, d - 1, :, :] = line_sum(p, lax.rem(z + d, zs))
            rz_copy(p, d).start()

    def scatter_end(p):
        value = line_sum(p, z)
        for d in range(1, zs):
            rz_copy(p, d).wait_recv()
            value += z_in[p, d - 1, :, :]
        here = pl.ds(p * piece, piece)
        out[here, :] = (tokens[here, :].astype(jnp.float32) + value).astype(out.dtype)

    for p in range(PASSES):
        normed[p, spot(x, z), :] = scaled[p * piece:(p + 1) * piece]
    gather_z(0)
    gather_x(0)
    gather_end(0)

    def chip_sum(u, chip):
        near = pl.ds(pl.multiple_of(chip * block, block), block)
        return part[u, mine(chip), :] + from_core[u, near, :]

    def step(j, carry):
        for p in range(1, PASSES):
            first = (p - 1) * TILES
            pl.when(j == first)(functools.partial(gather_z, p))
            pl.when(j == first + 4)(functools.partial(gather_x, p))
            pl.when(j == first + TILES)(functools.partial(gather_end, p))

        @pl.when(j < total_steps)
        def _():
            for copy in weights(j):
                copy.wait()

            @pl.when(j + 1 < total_steps)
            def _():
                for copy in weights(j + 1):
                    copy.start()

            slot, p = lax.rem(j, 2), j // TILES
            part[j, :, :width] = jnp.dot(normed[p], gate_buf[slot], preferred_element_type=jnp.float32)
            part[j, :, width:] = jnp.dot(normed[p], up_buf[slot], preferred_element_type=jnp.float32)
            core_copy(j).start()

        @pl.when((j >= 1) & (j < total_steps + 1))
        def _():
            u = j - 1
            core_copy(u).wait_recv()
            for d in range(1, chips):
                sums_out[u, d - 1, :, :] = chip_sum(u, peer(d))
                y_copy(u, d).start()

        @pl.when((j >= 2) & (j < total_steps + 2))
        def _():
            u = j - 2
            total = chip_sum(u, y)
            for d in range(1, chips):
                y_copy(u, d).wait_recv()
                total += sums_in[u, d - 1, :, :]
            hid[u, mine(y), :] = (jax.nn.silu(total[:, :width]) * total[:, width:]).astype(jnp.bfloat16)
            for d in range(1, chips):
                h_copy(u, d).start()
            p_copy(u, 0).start()

        @pl.when((j >= 3) & (j < total_steps + 3))
        def _():
            u = j - 3
            for d in range(1, chips):
                h_copy(u, d).wait_recv()
                p_copy(u, d).start()

        @pl.when(j >= 4)
        def _():
            u = j - 4
            p, t = u // TILES, lax.rem(u, TILES)
            down_weights(u).wait()

            @pl.when(u + 1 < total_steps)
            def _():
                down_weights(u + 1).start()

            for d in range(chips):
                p_copy(u, d).wait_recv()
            term = jnp.dot(hid[u], down_buf[lax.rem(u, 2)], preferred_element_type=jnp.float32)

            @pl.when(t == 0)
            def _():
                acc[p, :, :] = term

            @pl.when(t > 0)
            def _():
                acc[p, :, :] += term

        for p in range(PASSES - 1):
            last = (p + 1) * TILES + 3
            pl.when(j == last)(functools.partial(scatter_x, p))
            pl.when(j == last + 4)(functools.partial(scatter_z, p))
            pl.when(j == last + 7)(functools.partial(scatter_end, p))
        return carry

    lax.fori_loop(0, total_steps + 4, step, 0)

    scatter_x(PASSES - 1)
    scatter_z(PASSES - 1)
    scatter_end(PASSES - 1)

    for d in range(1, rows):
        s_copy(d).wait_send()
    for p in range(PASSES):
        for d in range(1, zs):
            ga_copy(p, d).wait_send()
            rz_copy(p, d).wait_send()
        for e in range(1, xs):
            gb_copy(p, e).wait_send()
            rx_copy(p, e).wait_send()

    def drain(u, carry):
        core_copy(u).wait_send()
        for d in range(1, chips):
            y_copy(u, d).wait_send()
            h_copy(u, d).wait_send()
        for d in range(chips):
            p_copy(u, d).wait_send()
        return carry

    lax.fori_loop(0, total_steps, drain, 0)


def local(tokens, norm_gain, gate_weight, up_weight, down_weight):
    rows, cols = lax.axis_size("row"), lax.axis_size("col")
    xs = max(x for x in range(1, cols + 1) if cols % x == 0 and x * x <= cols)
    zs = cols // xs
    count, depth = tokens.shape
    hidden, features = down_weight.shape
    width, piece = hidden // TILES, count // PASSES
    span, chips = cols * piece, rows // CORES
    half, block = span // CORES, span // rows
    steps = PASSES * TILES
    hbm = pl.BlockSpec(memory_space=pl.ANY)
    vmem = pl.BlockSpec(memory_space=pltpu.VMEM)
    dma = pltpu.SemaphoreType.DMA
    f32, bf16 = jnp.float32, jnp.bfloat16
    return pl.pallas_call(
        functools.partial(block_kernel, rows, xs, zs),
        out_shape=jax.ShapeDtypeStruct((count, features), bf16),
        in_specs=[vmem, vmem, hbm, hbm, hbm],
        out_specs=vmem,
        scratch_shapes=[
            pltpu.VMEM((count, 128), f32),
            pltpu.VMEM((rows - 1, count, 128), f32),
            pltpu.VMEM((PASSES, span, depth), bf16),
            pltpu.VMEM((2, depth, width), bf16),
            pltpu.VMEM((2, depth, width), bf16),
            pltpu.VMEM((2, width, features), bf16),
            pltpu.VMEM((steps, span, 2 * width), f32),
            pltpu.VMEM((steps, half, 2 * width), f32),
            pltpu.VMEM((steps, chips - 1, block, 2 * width), f32),
            pltpu.VMEM((steps, chips - 1, block, 2 * width), f32),
            pltpu.VMEM((steps, span, width), bf16),
            pltpu.VMEM((PASSES, span, features), f32),
            pltpu.VMEM((PASSES, xs - 1, zs * piece, features), f32),
            pltpu.VMEM((PASSES, zs - 1, piece, features), f32),
            pltpu.VMEM((PASSES, zs - 1, piece, features), f32),
            dma((rows - 1,)), dma((rows - 1,)),
            dma((PASSES, zs - 1)), dma((PASSES, zs - 1)),
            dma((PASSES, xs - 1)), dma((PASSES, xs - 1)),
            dma((2, 2)), dma((2,)),
            dma((steps,)), dma((steps,)),
            dma((steps, chips - 1)), dma((steps, chips - 1)),
            dma((steps, chips - 1)), dma((steps, chips - 1)),
            dma((steps, chips)), dma((steps, chips)),
            dma((PASSES, xs - 1)), dma((PASSES, xs - 1)),
            dma((PASSES, zs - 1)), dma((PASSES, zs - 1)),
        ],
        compiler_params=pltpu.CompilerParams(
            collective_id=1, has_side_effects=True, vmem_limit_bytes=VMEM_LIMIT),
        name="block",
    )(tokens, norm_gain[None, :], gate_weight, up_weight, down_weight)


def solution(mesh):
    placed = (P("col", "row"), P("row"), P("row", "col"), P("row", "col"), P("col", "row"))
    return jax.shard_map(
        local, mesh=mesh, in_specs=placed, out_specs=P("col", "row"), check_vma=False
    )
```

```python
import functools

import jax
import jax.numpy as jnp
from jax import lax
from jax.experimental import pallas as pl
from jax.experimental.pallas import tpu as pltpu
from jax.sharding import PartitionSpec as P

MESH = pl.DeviceIdType.MESH
D = 8192
TILES = 7
CORES = 2
PASSES = 4
LAG = 3
VMEM_LIMIT = 67043328


epsilon = 1e-05


def block_kernel(
    rows, xs, zs,
    tokens, gain, gate_hbm, up_hbm, down_hbm, out,
    squares_out, squares_in, normed, gate_buf, up_buf, down_buf, part, from_core, sums_out, sums_in, hid,
    acc, x_in, z_out, z_in,
    s_send, s_recv, ga_send, ga_recv, gb_send, gb_recv, w_sem, d_sem, core_send, core_recv, y_send, y_recv,
    h_send, h_recv, p_send, p_recv, rx_send, rx_recv, rz_send, rz_recv,
):
    chips = rows // CORES
    me = lax.axis_index("row")
    y, core = me // CORES, me % CORES
    partner = y * CORES + (1 - core)
    at = lax.axis_index("col")
    z, x = at // xs, at % xs
    count = tokens.shape[0]
    piece = count // PASSES
    line = zs * piece
    span = normed.shape[1]
    half, block = span // CORES, span // rows
    width = gate_buf.shape[2]
    total_steps = PASSES * TILES

    def remote(src, dst, send, recv, device):
        return pltpu.make_async_remote_copy(src, dst, send, recv, device_id=device, device_id_type=MESH)

    def peer(d):
        return lax.rem(y + d, chips)

    def z_peer(d):
        return {"col": lax.rem(z + d, zs) * xs + x}

    def x_peer(e):
        return {"col": z * xs + lax.rem(x + e, xs)}

    def spot(to_x, to_z):
        return pl.ds(pl.multiple_of(to_x * line + to_z * piece, piece), piece)

    def mine(chip):
        return pl.ds(pl.multiple_of(core * half + chip * block, block), block)

    def weights(u):
        slot = lax.rem(u, 2)
        columns = pl.ds(pl.multiple_of(lax.rem(u, TILES) * width, width), width)
        return (
            pltpu.make_async_copy(gate_hbm.at[:, columns], gate_buf.at[slot], w_sem.at[slot, 0]),
            pltpu.make_async_copy(up_hbm.at[:, columns], up_buf.at[slot], w_sem.at[slot, 1]),
        )

    def down_weights(u):
        slot = lax.rem(u, 2)
        lines = pl.ds(pl.multiple_of(lax.rem(u, TILES) * width, width), width)
        return pltpu.make_async_copy(down_hbm.at[lines, :], down_buf.at[slot], d_sem.at[slot])

    def s_copy(d):
        return remote(squares_out, squares_in.at[d - 1], s_send.at[d - 1], s_recv.at[d - 1],
                      {"row": lax.rem(me + d, rows)})

    def ga_copy(p, d):
        return remote(normed.at[p, spot(x, z)], normed.at[p, spot(x, z)],
                      ga_send.at[p, d - 1], ga_recv.at[p, d - 1], z_peer(d))

    def gb_copy(p, e, d):
        here = spot(x, lax.rem(z + zs - d, zs))
        return remote(normed.at[p, here], normed.at[p, here],
                      gb_send.at[p, e - 1, d], gb_recv.at[p, e - 1, d], x_peer(e))

    def rx_copy(p, e, d):
        to_z = lax.rem(z + d, zs)
        near = pl.ds(pl.multiple_of(to_z * piece, piece), piece)
        return remote(acc.at[p, spot(lax.rem(x + e, xs), to_z)], x_in.at[p, e - 1, near],
                      rx_send.at[p, e - 1, d], rx_recv.at[p, e - 1, d], x_peer(e))

    def rz_copy(p, d):
        return remote(z_out.at[p, d - 1], z_in.at[p, d - 1],
                      rz_send.at[p, d - 1], rz_recv.at[p, d - 1], z_peer(d))

    def core_copy(u):
        other = pl.ds(pl.multiple_of((1 - core) * half, half), half)
        return remote(part.at[u, other], from_core.at[u], core_send.at[u], core_recv.at[u], {"row": partner})

    def y_copy(u, d):
        return remote(sums_out.at[u, d - 1], sums_in.at[u, d - 1], y_send.at[u, d - 1], y_recv.at[u, d - 1],
                      {"row": peer(d) * CORES + core})

    def h_copy(u, d):
        return remote(hid.at[u, mine(y)], hid.at[u, mine(y)], h_send.at[u, d - 1], h_recv.at[u, d - 1],
                      {"row": peer(d) * CORES + core})

    def p_copy(u, d):
        source = lax.rem(y + chips - d, chips)
        return remote(hid.at[u, mine(source)], hid.at[u, mine(source)], p_send.at[u, d], p_recv.at[u, d],
                      {"row": partner})

    for copy in weights(0):
        copy.start()
    down_weights(0).start()

    values = tokens[...].astype(jnp.float32)
    own_squares = jnp.sum(values * values, axis=1, keepdims=True)
    squares_out[...] = jnp.broadcast_to(own_squares, squares_out.shape)

    barrier = pltpu.get_barrier_semaphore()
    for d in range(1, rows):
        pl.semaphore_signal(barrier, inc=1, device_id={"row": lax.rem(me + d, rows)}, device_id_type=MESH)
    for d in range(1, zs):
        pl.semaphore_signal(barrier, inc=1, device_id=z_peer(d), device_id_type=MESH)
    for e in range(1, xs):
        pl.semaphore_signal(barrier, inc=1, device_id=x_peer(e), device_id_type=MESH)
    pl.semaphore_wait(barrier, rows + zs + xs - 3)

    for d in range(1, rows):
        s_copy(d).start()
    squares = squares_out[...]
    for d in range(1, rows):
        s_copy(d).wait_recv()
        squares += squares_in[d - 1]
    factor = lax.rsqrt(squares[:, :1] / D + epsilon)
    scaled = (values * factor * gain[...]).astype(jnp.bfloat16)

    def gather_z(p):
        for d in range(1, zs):
            ga_copy(p, d).start()

    def gather_x(p):
        for d in range(zs):
            if d:
                ga_copy(p, d).wait_recv()
            for e in range(1, xs):
                gb_copy(p, e, d).start()

    def gather_end(p):
        for d in range(zs):
            for e in range(1, xs):
                gb_copy(p, e, d).wait_recv()

    def scatter_x(p):
        for d in (*range(1, zs), 0):
            for e in range(1, xs):
                rx_copy(p, e, d).start()

    def line_sum(p, to_z):
        value = acc[p, spot(x, to_z), :]
        near = pl.ds(pl.multiple_of(to_z * piece, piece), piece)
        for e in range(1, xs):
            value += x_in[p, e - 1, near, :]
        return value

    def scatter_z(p):
        for d in range(1, zs):
            for e in range(1, xs):
                rx_copy(p, e, d).wait_recv()
            z_out[p, d - 1, :, :] = line_sum(p, lax.rem(z + d, zs))
            rz_copy(p, d).start()

    def scatter_end(p):
        for e in range(1, xs):
            rx_copy(p, e, 0).wait_recv()
        value = line_sum(p, z)
        for d in range(1, zs):
            rz_copy(p, d).wait_recv()
            value += z_in[p, d - 1, :, :]
        here = pl.ds(p * piece, piece)
        out[here, :] = (tokens[here, :].astype(jnp.float32) + value).astype(out.dtype)

    for p in range(PASSES):
        normed[p, spot(x, z), :] = scaled[p * piece:(p + 1) * piece]
    gather_z(0)
    gather_x(0)
    gather_end(0)

    def chip_sum(u, chip):
        near = pl.ds(pl.multiple_of(chip * block, block), block)
        return part[u, mine(chip), :] + from_core[u, near, :]

    def step(j, carry):
        for p in range(1, PASSES):
            first = (p - 1) * TILES
            pl.when(j == first)(functools.partial(gather_z, p))
            pl.when(j == first + 3)(functools.partial(gather_x, p))
            pl.when(j == first + TILES)(functools.partial(gather_end, p))

        @pl.when(j < total_steps)
        def _():
            for copy in weights(j):
                copy.wait()

            @pl.when(j + 1 < total_steps)
            def _():
                for copy in weights(j + 1):
                    copy.start()

            slot, p = lax.rem(j, 2), j // TILES
            part[j, :, :width] = jnp.dot(normed[p], gate_buf[slot], preferred_element_type=jnp.float32)
            part[j, :, width:] = jnp.dot(normed[p], up_buf[slot], preferred_element_type=jnp.float32)
            core_copy(j).start()

        @pl.when((j >= 1) & (j < total_steps + 1))
        def _():
            u = j - 1
            core_copy(u).wait_recv()
            for d in range(1, chips):
                sums_out[u, d - 1, :, :] = chip_sum(u, peer(d))
                y_copy(u, d).start()

        @pl.when((j >= LAG) & (j < total_steps + LAG))
        def _():
            u = j - LAG
            total = chip_sum(u, y)
            for d in range(1, chips):
                y_copy(u, d).wait_recv()
                total += sums_in[u, d - 1, :, :]
            hid[u, mine(y), :] = (jax.nn.silu(total[:, :width]) * total[:, width:]).astype(jnp.bfloat16)
            for d in range(1, chips):
                h_copy(u, d).start()
            p_copy(u, 0).start()

        @pl.when((j >= LAG + 1) & (j < total_steps + LAG + 1))
        def _():
            u = j - LAG - 1
            for d in range(1, chips):
                h_copy(u, d).wait_recv()
                p_copy(u, d).start()

        @pl.when(j >= LAG + 2)
        def _():
            u = j - LAG - 2
            p, t = u // TILES, lax.rem(u, TILES)
            down_weights(u).wait()

            @pl.when(u + 1 < total_steps)
            def _():
                down_weights(u + 1).start()

            for d in range(chips):
                p_copy(u, d).wait_recv()
            term = jnp.dot(hid[u], down_buf[lax.rem(u, 2)], preferred_element_type=jnp.float32)

            @pl.when(t == 0)
            def _():
                acc[p, :, :] = term

            @pl.when(t > 0)
            def _():
                acc[p, :, :] += term

        for p in range(PASSES - 1):
            last = (p + 1) * TILES + LAG + 1
            pl.when(j == last)(functools.partial(scatter_x, p))
            pl.when(j == last + 4)(functools.partial(scatter_z, p))
            if p < PASSES - 2:
                pl.when(j == last + 10)(functools.partial(scatter_end, p))
        return carry

    lax.fori_loop(0, total_steps + LAG + 2, step, 0)

    scatter_x(PASSES - 1)
    scatter_end(PASSES - 2)
    scatter_z(PASSES - 1)
    scatter_end(PASSES - 1)

    for d in range(1, rows):
        s_copy(d).wait_send()
    for p in range(PASSES):
        for d in range(1, zs):
            ga_copy(p, d).wait_send()
            rz_copy(p, d).wait_send()
        for e in range(1, xs):
            for d in range(zs):
                gb_copy(p, e, d).wait_send()
                rx_copy(p, e, d).wait_send()

    def drain(u, carry):
        core_copy(u).wait_send()
        for d in range(1, chips):
            y_copy(u, d).wait_send()
            h_copy(u, d).wait_send()
        for d in range(chips):
            p_copy(u, d).wait_send()
        return carry

    lax.fori_loop(0, total_steps, drain, 0)


def local(tokens, norm_gain, gate_weight, up_weight, down_weight):
    rows, cols = lax.axis_size("row"), lax.axis_size("col")
    xs = max(x for x in range(1, cols + 1) if cols % x == 0 and x * x <= cols)
    zs = cols // xs
    count, depth = tokens.shape
    hidden, features = down_weight.shape
    width, piece = hidden // TILES, count // PASSES
    span, chips = cols * piece, rows // CORES
    half, block = span // CORES, span // rows
    steps = PASSES * TILES
    hbm = pl.BlockSpec(memory_space=pl.ANY)
    vmem = pl.BlockSpec(memory_space=pltpu.VMEM)
    dma = pltpu.SemaphoreType.DMA
    f32, bf16 = jnp.float32, jnp.bfloat16
    return pl.pallas_call(
        functools.partial(block_kernel, rows, xs, zs),
        out_shape=jax.ShapeDtypeStruct((count, features), bf16),
        in_specs=[vmem, vmem, hbm, hbm, hbm],
        out_specs=vmem,
        scratch_shapes=[
            pltpu.VMEM((count, 128), f32),
            pltpu.VMEM((rows - 1, count, 128), f32),
            pltpu.VMEM((PASSES, span, depth), bf16),
            pltpu.VMEM((2, depth, width), bf16),
            pltpu.VMEM((2, depth, width), bf16),
            pltpu.VMEM((2, width, features), bf16),
            pltpu.VMEM((steps, span, 2 * width), f32),
            pltpu.VMEM((steps, half, 2 * width), f32),
            pltpu.VMEM((steps, chips - 1, block, 2 * width), f32),
            pltpu.VMEM((steps, chips - 1, block, 2 * width), f32),
            pltpu.VMEM((steps, span, width), bf16),
            pltpu.VMEM((PASSES, span, features), f32),
            pltpu.VMEM((PASSES, xs - 1, zs * piece, features), f32),
            pltpu.VMEM((PASSES, zs - 1, piece, features), f32),
            pltpu.VMEM((PASSES, zs - 1, piece, features), f32),
            dma((rows - 1,)), dma((rows - 1,)),
            dma((PASSES, zs - 1)), dma((PASSES, zs - 1)),
            dma((PASSES, xs - 1, zs)), dma((PASSES, xs - 1, zs)),
            dma((2, 2)), dma((2,)),
            dma((steps,)), dma((steps,)),
            dma((steps, chips - 1)), dma((steps, chips - 1)),
            dma((steps, chips - 1)), dma((steps, chips - 1)),
            dma((steps, chips)), dma((steps, chips)),
            dma((PASSES, xs - 1, zs)), dma((PASSES, xs - 1, zs)),
            dma((PASSES, zs - 1)), dma((PASSES, zs - 1)),
        ],
        compiler_params=pltpu.CompilerParams(
            collective_id=1, has_side_effects=True, vmem_limit_bytes=VMEM_LIMIT),
        name="block",
    )(tokens, norm_gain[None, :], gate_weight, up_weight, down_weight)


def solution(mesh):
    placed = (P("col", "row"), P("row"), P("row", "col"), P("row", "col"), P("col", "row"))
    return jax.shard_map(
        local, mesh=mesh, in_specs=placed, out_specs=P("col", "row"), check_vma=False
    )
```

```python
import functools

import jax
import jax.numpy as jnp
from jax import lax
from jax.experimental import pallas as pl
from jax.experimental.pallas import tpu as pltpu
from jax.sharding import PartitionSpec as P

MESH = pl.DeviceIdType.MESH
D = 8192
TILES = 7
CORES = 2
PASSES = 4
LAG = 3
VMEM_LIMIT = 67043328


epsilon = 1e-05


def block_kernel(
    rows, xs, zs,
    tokens, gain, gate_hbm, up_hbm, down_hbm, out,
    squares_out, squares_in, normed, gate_buf, up_buf, down_buf, part, from_core, sums_out, sums_in, hid,
    acc, x_in, z_out, z_in,
    s_send, s_recv, ga_send, ga_recv, gb_send, gb_recv, w_sem, d_sem, core_send, core_recv, y_send, y_recv,
    h_send, h_recv, p_send, p_recv, rx_send, rx_recv, rz_send, rz_recv,
):
    chips = rows // CORES
    me = lax.axis_index("row")
    y, core = me // CORES, me % CORES
    partner = y * CORES + (1 - core)
    at = lax.axis_index("col")
    z, x = at // xs, at % xs
    count = tokens.shape[0]
    piece = count // PASSES
    line = zs * piece
    span = normed.shape[1]
    half, block = span // CORES, span // rows
    width = gate_buf.shape[2]
    total_steps = PASSES * TILES

    def remote(src, dst, send, recv, device):
        return pltpu.make_async_remote_copy(src, dst, send, recv, device_id=device, device_id_type=MESH)

    def peer(d):
        return lax.rem(y + d, chips)

    def z_peer(d):
        return {"col": lax.rem(z + d, zs) * xs + x}

    def x_peer(e):
        return {"col": z * xs + lax.rem(x + e, xs)}

    def spot(to_x, to_z):
        return pl.ds(pl.multiple_of(to_x * line + to_z * piece, piece), piece)

    def mine(chip):
        return pl.ds(pl.multiple_of(core * half + chip * block, block), block)

    def weights(u):
        slot = lax.rem(u, 2)
        columns = pl.ds(pl.multiple_of(lax.rem(u, TILES) * width, width), width)
        return (
            pltpu.make_async_copy(gate_hbm.at[:, columns], gate_buf.at[slot], w_sem.at[slot, 0]),
            pltpu.make_async_copy(up_hbm.at[:, columns], up_buf.at[slot], w_sem.at[slot, 1]),
        )

    def down_weights(u):
        slot = lax.rem(u, 2)
        lines = pl.ds(pl.multiple_of(lax.rem(u, TILES) * width, width), width)
        return pltpu.make_async_copy(down_hbm.at[lines, :], down_buf.at[slot], d_sem.at[slot])

    def s_copy(d):
        return remote(squares_out, squares_in.at[d - 1], s_send.at[d - 1], s_recv.at[d - 1],
                      {"row": lax.rem(me + d, rows)})

    def ga_copy(p, d):
        return remote(normed.at[p, spot(x, z)], normed.at[p, spot(x, z)],
                      ga_send.at[p, d - 1], ga_recv.at[p, d - 1], z_peer(d))

    def gb_copy(p, e, d):
        here = spot(x, lax.rem(z + zs - d, zs))
        return remote(normed.at[p, here], normed.at[p, here],
                      gb_send.at[p, e - 1, d], gb_recv.at[p, e - 1, d], x_peer(e))

    def rx_copy(p, e, d):
        to_z = lax.rem(z + d, zs)
        near = pl.ds(pl.multiple_of(to_z * piece, piece), piece)
        return remote(acc.at[p, spot(lax.rem(x + e, xs), to_z)], x_in.at[p, e - 1, near],
                      rx_send.at[p, e - 1, d], rx_recv.at[p, e - 1, d], x_peer(e))

    def rz_copy(p, d):
        return remote(z_out.at[p, d - 1], z_in.at[p, d - 1],
                      rz_send.at[p, d - 1], rz_recv.at[p, d - 1], z_peer(d))

    def core_copy(u):
        other = pl.ds(pl.multiple_of((1 - core) * half, half), half)
        return remote(part.at[u, other], from_core.at[u], core_send.at[u], core_recv.at[u], {"row": partner})

    def y_copy(u, d):
        return remote(sums_out.at[u, d - 1], sums_in.at[u, d - 1], y_send.at[u, d - 1], y_recv.at[u, d - 1],
                      {"row": peer(d) * CORES + core})

    def h_copy(u, d):
        return remote(hid.at[u, mine(y)], hid.at[u, mine(y)], h_send.at[u, d - 1], h_recv.at[u, d - 1],
                      {"row": peer(d) * CORES + core})

    def p_copy(u, d):
        source = lax.rem(y + chips - d, chips)
        return remote(hid.at[u, mine(source)], hid.at[u, mine(source)], p_send.at[u, d], p_recv.at[u, d],
                      {"row": partner})

    for copy in weights(0):
        copy.start()
    down_weights(0).start()

    values = tokens[...].astype(jnp.float32)
    own_squares = jnp.sum(values * values, axis=1, keepdims=True)
    squares_out[...] = jnp.broadcast_to(own_squares, squares_out.shape)

    barrier = pltpu.get_barrier_semaphore()
    for d in range(1, rows):
        pl.semaphore_signal(barrier, inc=1, device_id={"row": lax.rem(me + d, rows)}, device_id_type=MESH)
    for d in range(1, zs):
        pl.semaphore_signal(barrier, inc=1, device_id=z_peer(d), device_id_type=MESH)
    for e in range(1, xs):
        pl.semaphore_signal(barrier, inc=1, device_id=x_peer(e), device_id_type=MESH)
    pl.semaphore_wait(barrier, rows + zs + xs - 3)

    for d in range(1, rows):
        s_copy(d).start()
    squares = squares_out[...]
    for d in range(1, rows):
        s_copy(d).wait_recv()
        squares += squares_in[d - 1]
    factor = lax.rsqrt(squares[:, :1] / D + epsilon)
    scaled = (values * factor * gain[...]).astype(jnp.bfloat16)

    def gather_z(p):
        for d in range(1, zs):
            ga_copy(p, d).start()

    def gather_x(p):
        for d in range(zs):
            if d:
                ga_copy(p, d).wait_recv()
            for e in range(1, xs):
                gb_copy(p, e, d).start()

    def gather_end(p):
        for d in range(zs):
            for e in range(1, xs):
                gb_copy(p, e, d).wait_recv()

    def scatter_x(p):
        for d in (*range(1, zs), 0):
            for e in range(1, xs):
                rx_copy(p, e, d).start()

    def line_sum(p, to_z):
        value = acc[p, spot(x, to_z), :]
        near = pl.ds(pl.multiple_of(to_z * piece, piece), piece)
        for e in range(1, xs):
            value += x_in[p, e - 1, near, :]
        return value

    def scatter_z(p):
        for d in range(1, zs):
            for e in range(1, xs):
                rx_copy(p, e, d).wait_recv()
            z_out[p, d - 1, :, :] = line_sum(p, lax.rem(z + d, zs))
            rz_copy(p, d).start()

    def scatter_end(p):
        for e in range(1, xs):
            rx_copy(p, e, 0).wait_recv()
        value = line_sum(p, z)
        for d in range(1, zs):
            rz_copy(p, d).wait_recv()
            value += z_in[p, d - 1, :, :]
        here = pl.ds(p * piece, piece)
        out[here, :] = (tokens[here, :].astype(jnp.float32) + value).astype(out.dtype)

    for p in range(PASSES):
        normed[p, spot(x, z), :] = scaled[p * piece:(p + 1) * piece]
    gather_z(0)
    gather_x(0)
    gather_end(0)

    def chip_sum(u, chip):
        near = pl.ds(pl.multiple_of(chip * block, block), block)
        return part[u, mine(chip), :] + from_core[u, near, :]

    def step(j, carry):
        for p in range(1, PASSES):
            first = (p - 1) * TILES
            pl.when(j == first)(functools.partial(gather_z, p))
            pl.when(j == first + 3)(functools.partial(gather_x, p))
            pl.when(j == first + TILES)(functools.partial(gather_end, p))

        @pl.when(j < total_steps)
        def _():
            for copy in weights(j):
                copy.wait()

            @pl.when(j + 1 < total_steps)
            def _():
                for copy in weights(j + 1):
                    copy.start()

            slot, p = lax.rem(j, 2), j // TILES
            part[j, :, :width] = jnp.dot(normed[p], gate_buf[slot], preferred_element_type=jnp.float32)
            part[j, :, width:] = jnp.dot(normed[p], up_buf[slot], preferred_element_type=jnp.float32)
            core_copy(j).start()

        @pl.when((j >= 1) & (j < total_steps + 1))
        def _():
            u = j - 1
            core_copy(u).wait_recv()
            for d in range(1, chips):
                sums_out[u, d - 1, :, :] = chip_sum(u, peer(d))
                y_copy(u, d).start()

        @pl.when((j >= LAG) & (j < total_steps + LAG))
        def _():
            u = j - LAG
            total = chip_sum(u, y)
            for d in range(1, chips):
                y_copy(u, d).wait_recv()
                total += sums_in[u, d - 1, :, :]
            hid[u, mine(y), :] = (jax.nn.silu(total[:, :width]) * total[:, width:]).astype(jnp.bfloat16)
            for d in range(1, chips):
                h_copy(u, d).start()
            p_copy(u, 0).start()

        @pl.when((j >= LAG + 2) & (j < total_steps + LAG + 2))
        def _():
            u = j - LAG - 2
            for d in range(1, chips):
                h_copy(u, d).wait_recv()
                p_copy(u, d).start()

        @pl.when(j >= LAG + 3)
        def _():
            u = j - LAG - 3
            p, t = u // TILES, lax.rem(u, TILES)
            down_weights(u).wait()

            @pl.when(u + 1 < total_steps)
            def _():
                down_weights(u + 1).start()

            for d in range(chips):
                p_copy(u, d).wait_recv()
            term = jnp.dot(hid[u], down_buf[lax.rem(u, 2)], preferred_element_type=jnp.float32)

            @pl.when(t == 0)
            def _():
                acc[p, :, :] = term

            @pl.when(t > 0)
            def _():
                acc[p, :, :] += term

        for p in range(PASSES - 1):
            last = (p + 1) * TILES + LAG + 2
            pl.when(j == last)(functools.partial(scatter_x, p))
            pl.when(j == last + 4)(functools.partial(scatter_z, p))
            if p < PASSES - 2:
                pl.when(j == last + 10)(functools.partial(scatter_end, p))
        return carry

    lax.fori_loop(0, total_steps + LAG + 3, step, 0)

    scatter_x(PASSES - 1)
    scatter_end(PASSES - 2)
    scatter_z(PASSES - 1)
    scatter_end(PASSES - 1)

    for d in range(1, rows):
        s_copy(d).wait_send()
    for p in range(PASSES):
        for d in range(1, zs):
            ga_copy(p, d).wait_send()
            rz_copy(p, d).wait_send()
        for e in range(1, xs):
            for d in range(zs):
                gb_copy(p, e, d).wait_send()
                rx_copy(p, e, d).wait_send()

    def drain(u, carry):
        core_copy(u).wait_send()
        for d in range(1, chips):
            y_copy(u, d).wait_send()
            h_copy(u, d).wait_send()
        for d in range(chips):
            p_copy(u, d).wait_send()
        return carry

    lax.fori_loop(0, total_steps, drain, 0)


def local(tokens, norm_gain, gate_weight, up_weight, down_weight):
    rows, cols = lax.axis_size("row"), lax.axis_size("col")
    xs = max(x for x in range(1, cols + 1) if cols % x == 0 and x * x <= cols)
    zs = cols // xs
    count, depth = tokens.shape
    hidden, features = down_weight.shape
    width, piece = hidden // TILES, count // PASSES
    span, chips = cols * piece, rows // CORES
    half, block = span // CORES, span // rows
    steps = PASSES * TILES
    hbm = pl.BlockSpec(memory_space=pl.ANY)
    vmem = pl.BlockSpec(memory_space=pltpu.VMEM)
    dma = pltpu.SemaphoreType.DMA
    f32, bf16 = jnp.float32, jnp.bfloat16
    return pl.pallas_call(
        functools.partial(block_kernel, rows, xs, zs),
        out_shape=jax.ShapeDtypeStruct((count, features), bf16),
        in_specs=[vmem, vmem, hbm, hbm, hbm],
        out_specs=vmem,
        scratch_shapes=[
            pltpu.VMEM((count, 128), f32),
            pltpu.VMEM((rows - 1, count, 128), f32),
            pltpu.VMEM((PASSES, span, depth), bf16),
            pltpu.VMEM((2, depth, width), bf16),
            pltpu.VMEM((2, depth, width), bf16),
            pltpu.VMEM((2, width, features), bf16),
            pltpu.VMEM((steps, span, 2 * width), f32),
            pltpu.VMEM((steps, half, 2 * width), f32),
            pltpu.VMEM((steps, chips - 1, block, 2 * width), f32),
            pltpu.VMEM((steps, chips - 1, block, 2 * width), f32),
            pltpu.VMEM((steps, span, width), bf16),
            pltpu.VMEM((PASSES, span, features), f32),
            pltpu.VMEM((PASSES, xs - 1, zs * piece, features), f32),
            pltpu.VMEM((PASSES, zs - 1, piece, features), f32),
            pltpu.VMEM((PASSES, zs - 1, piece, features), f32),
            dma((rows - 1,)), dma((rows - 1,)),
            dma((PASSES, zs - 1)), dma((PASSES, zs - 1)),
            dma((PASSES, xs - 1, zs)), dma((PASSES, xs - 1, zs)),
            dma((2, 2)), dma((2,)),
            dma((steps,)), dma((steps,)),
            dma((steps, chips - 1)), dma((steps, chips - 1)),
            dma((steps, chips - 1)), dma((steps, chips - 1)),
            dma((steps, chips)), dma((steps, chips)),
            dma((PASSES, xs - 1, zs)), dma((PASSES, xs - 1, zs)),
            dma((PASSES, zs - 1)), dma((PASSES, zs - 1)),
        ],
        compiler_params=pltpu.CompilerParams(
            collective_id=1, has_side_effects=True, vmem_limit_bytes=VMEM_LIMIT),
        name="block",
    )(tokens, norm_gain[None, :], gate_weight, up_weight, down_weight)


def solution(mesh):
    placed = (P("col", "row"), P("row"), P("row", "col"), P("row", "col"), P("col", "row"))
    return jax.shard_map(
        local, mesh=mesh, in_specs=placed, out_specs=P("col", "row"), check_vma=False
    )
```
